32 devices in a mesh: rows: 8 (over y, x, core), dim: 4 (over z).
Axes of the slice: x: 2, y: 2, z: 4, core: 2. Of those that a mesh axis runs over, the one named last changes fastest.
Arguments:
- entity_table: float32 [131072, 512], P(('rows', 'dim')), may hold values from -2.5 to 2.5
- relations: float32 [822, 512], replicated, may hold values from -6 to 6
- thresholds: float32 [64], replicated, may hold values from 0.2 to 2
- head_ids: int32 [2048], replicated, may hold values from 0 to 131071
- rel_ids: int32 [2048], replicated, may hold values from 0 to 821
- thr_idx: int32 [2048], replicated, may hold values from 0 to 63
Outputs:
- serving_table: float32 [131072, 512], P('rows', 'dim')
- fraction: float32 [2048], P(('rows', 'dim'))
The draws below stay inside these ranges and needn't reach their ends.
All inputs are finite; a program needn't handle non-finite values.
Results may differ from the reference program's by a relative error of at most 0.0011.
Values sent between devices are 32-bit elements; how exact they have to be, the bound alone decides.
A program may use at most 128 MiB of HBM per device.

```python
import math
import jax
import jax.numpy as jnp
from jax import lax

D = 512
ENT_DEV = 4096
Q = 2048
NREL = 822
NTHR = 64
ENT = 131072


cluster_count = 32


def draw_entity_table(key, part):
    key_ids = jax.random.fold_in(key, 11)
    key_cent = jax.random.fold_in(key, 12)
    key_vals = jax.random.fold_in(key, 13)
    key_jit = jax.random.fold_in(key, 14)
    member = jax.random.randint(key_ids, (ENT,), 0, cluster_count)
    centers = jnp.clip(jax.random.normal(key_cent, (cluster_count, D), jnp.float32), -6.0, 6.0)
    shared = jnp.take(centers, member, axis=0)
    position = jnp.arange(ENT, dtype=jnp.float32)[:, None] / ENT
    jitter = jax.random.uniform(key_jit, (ENT, 1), jnp.float32, -0.5, 0.5)
    scale = float(D) ** (-0.25) * jnp.exp(math.log(3.0) * (position - 0.5) + jitter)
    noise = jnp.clip(jax.random.normal(key_vals, (ENT, D), jnp.float32), -6.0, 6.0)
    values = scale * (0.8 * shared + 0.6 * noise)
    return jnp.clip(values, -2.5, 2.5).astype(jnp.float32)


def place_ends(drawn, rng, least, top_value):
    spot = [jax.random.randint(jax.random.fold_in(rng, axis), (), 0, length) for axis, length in enumerate(drawn.shape)]
    widest = drawn.shape.index(max(drawn.shape))
    beside = spot[:widest] + [(spot[widest] + 1) % drawn.shape[widest]] + spot[widest + 1:]
    return drawn.at[tuple(spot)].set(least).at[tuple(beside)].set(top_value)


def scatter_about(stream_key, extent, deviation, reach, held_as=jnp.bfloat16):
    result = deviation * jax.random.normal(stream_key, extent, jnp.float32)
    return jnp.clip(result, min=-reach, max=reach).astype(held_as)


def setup_inputs(seed: int = 0) -> dict:
    key_of = jax.random.split(jax.random.key(seed), 7)
    return {
        "entity_table": draw_entity_table(jax.random.fold_in(key_of[6], 71), 0),
        "relations": scatter_about(key_of[1], (NREL, D), 1.0, 6.0, jnp.float32),
        "thresholds": jnp.clip(jax.random.uniform(key_of[2], (NTHR,), jnp.float32, 0.2, 2.0), 0.2, 2.0),
        "head_ids": place_ends(jax.random.randint(key_of[3], (Q,), 0, ENT), jax.random.fold_in(key_of[3], 1), 0, ENT - 1).astype(jnp.int32),
        "rel_ids": place_ends(jax.random.randint(key_of[4], (Q,), 0, NREL), jax.random.fold_in(key_of[4], 1), 0, NREL - 1).astype(jnp.int32),
        "thr_idx": place_ends(jax.random.randint(key_of[5], (Q,), 0, NTHR), jax.random.fold_in(key_of[5], 1), 0, NTHR - 1).astype(jnp.int32),
    }


sharpness = 2.0


def reference(entity_table, relations, thresholds, head_ids, rel_ids, thr_idx):
    head_vecs = jnp.take(entity_table, head_ids, axis=0)
    query = (head_vecs * jnp.take(relations, rel_ids, axis=0)).astype(jnp.bfloat16)
    query = lax.optimization_barrier(query).astype(jnp.float32)
    level = jnp.take(thresholds, thr_idx)
    block = ENT_DEV * 4
    count = ENT // block
    blocks = entity_table.reshape(count, block, D)

    def step(total, rows_block):
        ent_low = lax.optimization_barrier(rows_block.astype(jnp.bfloat16)).astype(jnp.float32)
        score = jnp.dot(query, ent_low.T, precision=lax.Precision.HIGHEST, preferred_element_type=jnp.float32)
        soft = jax.nn.sigmoid(sharpness * (score - level[:, None]))
        return total + jnp.sum(soft, axis=1), None

    total, unused = lax.scan(step, jnp.zeros((Q,), jnp.float32), blocks)
    return entity_table, total * (1.0 / ENT)
```

```python
import functools
import jax
import jax.numpy as jnp
from jax import lax
from jax.sharding import PartitionSpec as P
from jax.experimental import pallas as pl
from jax.experimental.pallas import tpu as pltpu

MESH = pl.DeviceIdType.MESH
sharpness = 2.0
lanes = 128
units = 16


def plan_for(size):
    middles = 2 * bits_of(size) - 1
    entry = 4
    middle = min(2, (units - entry - 1) // middles)
    return (entry,) + (middle,) * middles + (units - entry - middle * middles,)


def bits_of(size):
    assert size & (size - 1) == 0
    return size.bit_length() - 1


def kernel(
    R, N, total_ents, head_ids, rel_ids, thr, thr_idx, rel, table, *others
):
    slabs = others[:-23]
    (
        serving, frac_out,
        tab, low, part, recv, full, qb, lev, frac, fr_rows, fr_dim, fr_sum,
        load_sem, own_sem, a2a_send, a2a_recv, ex_send, ex_recv, f_send, f_recv, g_send, g_recv,
    ) = others[-23:]
    r = lax.axis_index("rows")
    d = lax.axis_index("dim")
    n, width = table.shape
    slab = width // N
    Q = part.shape[0]
    half_q = Q // 2
    chunk = n // units
    plan = plan_for(N)

    load = pltpu.make_async_copy(table, tab, load_sem)
    load.start()

    row_peers = [lax.rem(r + k, R) for k in range(1, R)]
    dim_peers = [lax.rem(d + k, N) for k in range(1, N)]
    barrier = pltpu.get_barrier_semaphore()
    for t in row_peers:
        pl.semaphore_signal(barrier, inc=1, device_id=(t, d), device_id_type=MESH)
    for t in dim_peers:
        pl.semaphore_signal(barrier, inc=1, device_id=(r, t), device_id_type=MESH)
    pl.semaphore_wait(barrier, R + N - 2)

    def slab_rows(source, t, start, rows):
        if slabs:
            return slabs[0].at[t, pl.ds(start, rows), :]
        return source.at[pl.ds(start, rows), pl.ds(pl.multiple_of(t * slab, slab), slab)]

    a2a = []
    starts = [sum(plan[:i]) * chunk for i in range(len(plan))]

    def issue(piece):
        rows = plan[piece] * chunk
        for k, t in enumerate(dim_peers):
            copy = pltpu.make_async_remote_copy(
                src_ref=slab_rows(table, t, starts[piece], rows),
                dst_ref=serving.at[pl.ds(pl.multiple_of(d * n + starts[piece], 8), rows), :],
                send_sem=a2a_send.at[piece, k],
                recv_sem=a2a_recv.at[piece, k],
                device_id=(r, t),
                device_id_type=MESH,
            )
            copy.start()
            a2a.append(copy)

    issue(0)

    load.wait()
    own = pltpu.make_async_copy(
        slab_rows(tab, d, 0, n),
        serving.at[pl.ds(pl.multiple_of(d * n, 8), n), :],
        own_sem,
    )
    own.start()
    first = (r * N + d) * n

    def pick(i, carry):
        base = pl.multiple_of(i * 8, 8)
        rows = []
        for j in range(8):
            local = head_ids[base + j] - first
            owned = jnp.logical_and(local >= 0, local < n)
            row = tab[pl.ds(jnp.clip(local, 0, n - 1), 1), :]
            rows.append(jnp.where(owned, row, jnp.zeros_like(row)))
        part[pl.ds(base, 8), :] = jnp.concatenate(rows, axis=0)
        return carry

    lax.fori_loop(0, Q // 8, pick, 0)

    row_bits = [("rows", b) for b in range(bits_of(R))]
    dim_bits = [("dim", b) for b in range(bits_of(N))]
    orders = [row_bits + dim_bits, row_bits[:1] + row_bits[:0:-1] + dim_bits]
    steps = len(orders[0])
    nrow = len(row_bits)

    def bit_and_peer(axis, b):
        me = r if axis == "rows" else d
        bit = lax.rem(me // (2 ** b), 2)
        other = me + (1 - 2 * bit) * (2 ** b)
        return bit, ((other, d) if axis == "rows" else (r, other))

    def exchange(src, dst, peer, stream, slot):
        copy = pltpu.make_async_remote_copy(
            src_ref=src, dst_ref=dst,
            send_sem=ex_send.at[stream, slot], recv_sem=ex_recv.at[stream, slot],
            device_id=peer, device_id_type=MESH,
        )
        copy.start()
        return copy

    offset = [0, half_q]
    size = half_q
    into = 0
    piece = 1
    for k in range(steps):
        h = size // 2
        copies = []
        for s in range(2):
            bit, peer = bit_and_peer(*orders[s][k])
            gone = pl.multiple_of(offset[s] + (1 - bit) * h, 8)
            copies.append(exchange(
                part.at[pl.ds(gone, h), :],
                recv.at[pl.ds(s * half_q + into, h), :],
                peer, s, k,
            ))
            offset[s] = pl.multiple_of(offset[s] + bit * h, 8)
        if k >= nrow:
            if piece < len(plan) - 1:
                issue(piece)
                piece += 1
        if k == 0:
            def narrow(i, carry):
                at = pl.multiple_of(i * 128, 128)
                low[pl.ds(at, 128), :] = tab[pl.ds(at, 128), :].astype(jnp.bfloat16)
                return carry

            lax.fori_loop(0, n // 128, narrow, 0)
        if k == 1:
            idx = thr_idx[...]

            def choose(t, acc):
                return jnp.where(idx == t, thr[t], acc)

            lev[...] = lax.fori_loop(0, thr.shape[0], choose, jnp.zeros(idx.shape, jnp.float32))
        for s in range(2):
            copies[s].wait()
            if h >= 64:
                def add(i, carry, s=s, into=into):
                    at = pl.ds(pl.multiple_of(offset[s] + i * 64, 8), 64)
                    frm = pl.ds(s * half_q + into + i * 64, 64)
                    part[at, :] = part[at, :] + recv[frm, :]
                    return carry

                lax.fori_loop(0, h // 64, add, 0)
            else:
                at = pl.ds(offset[s], h)
                part[at, :] = part[at, :] + recv[pl.ds(s * half_q + into, h), :]
        into += h
        size = h

    for s in range(2):
        def form(i, carry, s=s):
            base = pl.multiple_of(offset[s] + i * 8, 8)
            rows = [rel[pl.ds(rel_ids[base + j], 1), :] for j in range(8)]
            full[pl.ds(base, 8), :] = part[pl.ds(base, 8), :] * jnp.concatenate(rows, axis=0)
            return carry

        lax.fori_loop(0, size // 8, form, 0)

    def count_pair(q0, q1):
        qb[:lanes, :] = full[pl.ds(q0, lanes), :].astype(jnp.bfloat16)
        qb[lanes:, :] = full[pl.ds(q1, lanes), :].astype(jnp.bfloat16)
        i0 = q0 // lanes
        i1 = q1 // lanes
        level = jnp.concatenate([lev[i0], lev[i1]], axis=1)
        rows = 512

        def tile(i, acc):
            at = pl.multiple_of(i * rows, rows)
            score = lax.dot_general(
                low[pl.ds(at, rows), :], qb[...], (((1,), (1,)), ((), ())),
                preferred_element_type=jnp.float32,
            )
            soft = jax.nn.sigmoid(sharpness * (score - level))
            return acc + jnp.sum(soft.reshape(rows // 8, 8, 2 * lanes), axis=0)

        acc = lax.fori_loop(0, n // rows, tile, jnp.zeros((8, 2 * lanes), jnp.float32))
        share = jnp.sum(acc, axis=0, keepdims=True) * (1.0 / total_ents)
        frac[i0] = share[:, :lanes]
        frac[i1] = share[:, lanes:]

    def count(starts_, rows):
        def body(i, carry):
            count_pair(pl.multiple_of(starts_[0] + i * lanes, lanes), pl.multiple_of(starts_[1] + i * lanes, lanes))
            return carry

        lax.fori_loop(0, rows // lanes, body, 0)

    pending = None
    counted = False
    slot = steps
    for k in reversed(range(steps)):
        copies = []
        there = []
        for s in range(2):
            bit, peer = bit_and_peer(*orders[s][k])
            here = full.at[pl.ds(offset[s], size), :]
            copies.append(exchange(here, here, peer, s, slot))
            there.append(pl.multiple_of(offset[s] + (1 - 2 * bit) * size, 8))
            offset[s] = pl.multiple_of(offset[s] - bit * size, 8)
        slot += 1
        if k >= nrow:
            issue(piece)
            piece += 1
        if pending is not None:
            count(*pending)
            pending = None
        for copy in copies:
            copy.wait()
        size = 2 * size
        if k <= nrow and size >= lanes:
            pending = (there, size // 2) if counted else (list(offset), size)
            counted = True
    count(*pending)

    per = frac.shape[0] // R
    sends = []
    for k, t in enumerate(row_peers):
        copy = pltpu.make_async_remote_copy(
            src_ref=frac.at[pl.ds(t * per, per)],
            dst_ref=fr_rows.at[R - 2 - k],
            send_sem=f_send.at[k], recv_sem=f_recv.at[R - 2 - k],
            device_id=(t, d), device_id_type=MESH,
        )
        copy.start()
        sends.append(copy)
    total = frac[pl.ds(r * per, per)]
    for k in range(R - 1):
        sends[k].wait_send()
        pltpu.make_async_remote_copy(
            src_ref=frac.at[pl.ds(r * per, per)],
            dst_ref=fr_rows.at[k], send_sem=f_send.at[k], recv_sem=f_recv.at[k],
            device_id=(row_peers[k], d), device_id_type=MESH,
        ).wait_recv()
        total = total + fr_rows[k]
    fr_sum[...] = total
    sends = []
    for k, t in enumerate(dim_peers):
        copy = pltpu.make_async_remote_copy(
            src_ref=fr_sum, dst_ref=fr_dim.at[N - 2 - k],
            send_sem=g_send.at[k], recv_sem=g_recv.at[N - 2 - k],
            device_id=(r, t), device_id_type=MESH,
        )
        copy.start()
        sends.append(copy)
    for k in range(N - 1):
        sends[k].wait_send()
        pltpu.make_async_remote_copy(
            src_ref=fr_sum, dst_ref=fr_dim.at[k],
            send_sem=g_send.at[k], recv_sem=g_recv.at[k],
            device_id=(r, dim_peers[k]), device_id_type=MESH,
        ).wait_recv()
        total = total + fr_dim[k]
    frac_out[...] = total
    own.wait()
    for copy in a2a:
        copy.wait()


def shards(entity_table, relations, thresholds, head_ids, rel_ids, thr_idx):
    R = lax.axis_size("rows")
    N = lax.axis_size("dim")
    n, width = entity_table.shape
    Q = head_ids.shape[0]
    blocks = Q // lanes
    per = blocks // R
    steps = bits_of(R) + bits_of(N)
    pieces = len(plan_for(N))
    f32 = jnp.float32
    DMA = pltpu.SemaphoreType.DMA
    smem = pl.BlockSpec(memory_space=pltpu.SMEM)
    vmem = pl.BlockSpec(memory_space=pltpu.VMEM)
    hbm = pl.BlockSpec(memory_space=pl.ANY)
    operands = [head_ids, rel_ids, thresholds, thr_idx.reshape(blocks, 1, lanes), relations, entity_table]
    if (width // N) % lanes:
        operands.append(entity_table.reshape(n, N, width // N).transpose(1, 0, 2))
    serving, share = pl.pallas_call(
        functools.partial(kernel, R, N, n * R * N),
        out_shape=(
            jax.ShapeDtypeStruct((n * N, width // N), f32),
            jax.ShapeDtypeStruct((per, 1, lanes), f32),
        ),
        in_specs=[smem, smem, smem, vmem, vmem] + [hbm] * (len(operands) - 5),
        out_specs=(hbm, vmem),
        scratch_shapes=[
            pltpu.VMEM((n, width), f32),
            pltpu.VMEM((n, width), jnp.bfloat16),
            pltpu.VMEM((Q, width), f32),
            pltpu.VMEM((Q, width), f32),
            pltpu.VMEM((Q, width), f32),
            pltpu.VMEM((2 * lanes, width), jnp.bfloat16),
            pltpu.VMEM((blocks, 1, lanes), f32),
            pltpu.VMEM((blocks, 1, lanes), f32),
            pltpu.VMEM((R - 1, per, 1, lanes), f32),
            pltpu.VMEM((N - 1, per, 1, lanes), f32),
            pltpu.VMEM((per, 1, lanes), f32),
            DMA, DMA,
            DMA((pieces, N - 1)), DMA((pieces, N - 1)),
            DMA((2, 2 * steps)), DMA((2, 2 * steps)),
            DMA((R - 1,)), DMA((R - 1,)),
            DMA((N - 1,)), DMA((N - 1,)),
        ],
        compiler_params=pltpu.CompilerParams(
            collective_id=0, has_side_effects=True, vmem_limit_bytes=60 * 2**20
        ),
    )(*operands)
    mine = Q // (R * N)
    fraction = lax.dynamic_slice(share.reshape(Q // R), (lax.axis_index("dim") * mine,), (mine,))
    return serving, fraction


def solution(mesh):
    placed = (P(("rows", "dim"), None), P(), P(), P(), P(), P())
    return jax.shard_map(
        shards,
        mesh=mesh,
        in_specs=placed,
        out_specs=(P("rows", "dim"), P(("rows", "dim"))),
        check_vma=False,
    )
```

```python
import functools
import jax
import jax.numpy as jnp
from jax import lax
from jax.sharding import PartitionSpec as P
from jax.experimental import pallas as pl
from jax.experimental.pallas import tpu as pltpu

MESH = pl.DeviceIdType.MESH
sharpness = 2.0
lanes = 128
units = 16


def plan_for(size):
    middles = 2 * bits_of(size) - 1
    entry = 4
    middle = min(2, (units - entry - 1) // middles)
    return (entry,) + (middle,) * middles + (units - entry - middle * middles,)


def bits_of(size):
    assert size & (size - 1) == 0
    return size.bit_length() - 1


def flipped(index, mask):
    out = index
    for b in range(mask.bit_length()):
        if (mask >> b) & 1:
            out = out + (1 - 2 * lax.rem(index // (2 ** b), 2)) * (2 ** b)
    return out


def kernel(
    R, N, total_ents, head_ids, rel_ids, thr, thr_idx, rel, table, *others
):
    slabs = others[:-23]
    (
        serving, frac_out,
        tab, low, part, recv, full, qb, lev, frac, fr_rows, fr_dim, fr_sum,
        load_sem, own_sem, a2a_send, a2a_recv, ex_send, ex_recv, f_send, f_recv, g_send, g_recv,
    ) = others[-23:]
    r = lax.axis_index("rows")
    d = lax.axis_index("dim")
    n, width = table.shape
    slab = width // N
    Q = part.shape[0]
    half_q = Q // 2
    chunk = n // units
    plan = plan_for(N)

    load = pltpu.make_async_copy(table, tab, load_sem)
    load.start()

    row_peers = [lax.rem(r + k, R) for k in range(1, R)]
    dim_peers = [flipped(d, k) for k in range(1, N)]
    barrier = pltpu.get_barrier_semaphore()
    for t in row_peers:
        pl.semaphore_signal(barrier, inc=1, device_id=(t, d), device_id_type=MESH)
    for t in dim_peers:
        pl.semaphore_signal(barrier, inc=1, device_id=(r, t), device_id_type=MESH)
    pl.semaphore_wait(barrier, R + N - 2)

    def slab_rows(source, t, start, rows):
        if slabs:
            return slabs[0].at[t, pl.ds(start, rows), :]
        return source.at[pl.ds(start, rows), pl.ds(pl.multiple_of(t * slab, slab), slab)]

    a2a = []
    starts = [sum(plan[:i]) * chunk for i in range(len(plan))]

    def issue(piece):
        rows = plan[piece] * chunk
        for k, t in enumerate(dim_peers):
            copy = pltpu.make_async_remote_copy(
                src_ref=slab_rows(table, t, starts[piece], rows),
                dst_ref=serving.at[pl.ds(pl.multiple_of(d * n + starts[piece], 8), rows), :],
                send_sem=a2a_send.at[piece, k],
                recv_sem=a2a_recv.at[piece, k],
                device_id=(r, t),
                device_id_type=MESH,
            )
            copy.start()
            a2a.append(copy)

    issue(0)

    load.wait()
    own = pltpu.make_async_copy(
        slab_rows(tab, d, 0, n),
        serving.at[pl.ds(pl.multiple_of(d * n, 8), n), :],
        own_sem,
    )
    own.start()
    first = (r * N + d) * n

    def pick(i, carry):
        base = pl.multiple_of(i * 8, 8)
        rows = []
        for j in range(8):
            local = head_ids[base + j] - first
            owned = jnp.logical_and(local >= 0, local < n)
            row = tab[pl.ds(jnp.clip(local, 0, n - 1), 1), :]
            rows.append(jnp.where(owned, row, jnp.zeros_like(row)))
        part[pl.ds(base, 8), :] = jnp.concatenate(rows, axis=0)
        return carry

    lax.fori_loop(0, Q // 8, pick, 0)

    row_bits = [("rows", b) for b in range(bits_of(R))]
    dim_bits = [("dim", b) for b in range(bits_of(N))]
    orders = [row_bits + dim_bits, row_bits[:1] + row_bits[:0:-1] + dim_bits]
    steps = len(orders[0])
    nrow = len(row_bits)

    def bit_and_peer(axis, b):
        me = r if axis == "rows" else d
        bit = lax.rem(me // (2 ** b), 2)
        other = me + (1 - 2 * bit) * (2 ** b)
        return bit, ((other, d) if axis == "rows" else (r, other))

    def exchange(src, dst, peer, stream, slot):
        copy = pltpu.make_async_remote_copy(
            src_ref=src, dst_ref=dst,
            send_sem=ex_send.at[stream, slot], recv_sem=ex_recv.at[stream, slot],
            device_id=peer, device_id_type=MESH,
        )
        copy.start()
        return copy

    offset = [0, half_q]
    size = half_q
    into = 0
    piece = 1
    for k in range(steps):
        h = size // 2
        copies = []
        for s in range(2):
            bit, peer = bit_and_peer(*orders[s][k])
            gone = pl.multiple_of(offset[s] + (1 - bit) * h, 8)
            copies.append(exchange(
                part.at[pl.ds(gone, h), :],
                recv.at[pl.ds(s * half_q + into, h), :],
                peer, s, k,
            ))
            offset[s] = pl.multiple_of(offset[s] + bit * h, 8)
        if k >= nrow:
            if piece < len(plan) - 1:
                issue(piece)
                piece += 1
        if k == 0:
            def narrow(i, carry):
                at = pl.multiple_of(i * 128, 128)
                low[pl.ds(at, 128), :] = tab[pl.ds(at, 128), :].astype(jnp.bfloat16)
                return carry

            lax.fori_loop(0, n // 128, narrow, 0)
        if k == 1:
            idx = thr_idx[...]

            def choose(t, acc):
                return jnp.where(idx == t, thr[t], acc)

            lev[...] = lax.fori_loop(0, thr.shape[0], choose, jnp.zeros(idx.shape, jnp.float32))
        for s in range(2):
            copies[s].wait()
            if h >= 64:
                def add(i, carry, s=s, into=into):
                    at = pl.ds(pl.multiple_of(offset[s] + i * 64, 8), 64)
                    frm = pl.ds(s * half_q + into + i * 64, 64)
                    part[at, :] = part[at, :] + recv[frm, :]
                    return carry

                lax.fori_loop(0, h // 64, add, 0)
            else:
                at = pl.ds(offset[s], h)
                part[at, :] = part[at, :] + recv[pl.ds(s * half_q + into, h), :]
        into += h
        size = h

    for s in range(2):
        def form(i, carry, s=s):
            base = pl.multiple_of(offset[s] + i * 8, 8)
            rows = [rel[pl.ds(rel_ids[base + j], 1), :] for j in range(8)]
            full[pl.ds(base, 8), :] = part[pl.ds(base, 8), :] * jnp.concatenate(rows, axis=0)
            return carry

        lax.fori_loop(0, size // 8, form, 0)

    def count_pair(q0, q1):
        qb[:lanes, :] = full[pl.ds(q0, lanes), :].astype(jnp.bfloat16)
        qb[lanes:, :] = full[pl.ds(q1, lanes), :].astype(jnp.bfloat16)
        i0 = q0 // lanes
        i1 = q1 // lanes
        level = jnp.concatenate([lev[i0], lev[i1]], axis=1)
        rows = 512

        def tile(i, acc):
            at = pl.multiple_of(i * rows, rows)
            score = lax.dot_general(
                low[pl.ds(at, rows), :], qb[...], (((1,), (1,)), ((), ())),
                preferred_element_type=jnp.float32,
            )
            soft = jax.nn.sigmoid(sharpness * (score - level))
            return acc + jnp.sum(soft.reshape(rows // 8, 8, 2 * lanes), axis=0)

        acc = lax.fori_loop(0, n // rows, tile, jnp.zeros((8, 2 * lanes), jnp.float32))
        share = jnp.sum(acc, axis=0, keepdims=True) * (1.0 / total_ents)
        frac[i0] = share[:, :lanes]
        frac[i1] = share[:, lanes:]

    def count(starts_, rows):
        def body(i, carry):
            count_pair(pl.multiple_of(starts_[0] + i * lanes, lanes), pl.multiple_of(starts_[1] + i * lanes, lanes))
            return carry

        lax.fori_loop(0, rows // lanes, body, 0)

    pending = None
    counted = False
    slot = steps
    for k in reversed(range(steps)):
        copies = []
        there = []
        for s in range(2):
            bit, peer = bit_and_peer(*orders[s][k])
            here = full.at[pl.ds(offset[s], size), :]
            copies.append(exchange(here, here, peer, s, slot))
            there.append(pl.multiple_of(offset[s] + (1 - 2 * bit) * size, 8))
            offset[s] = pl.multiple_of(offset[s] - bit * size, 8)
        slot += 1
        if k >= nrow:
            issue(piece)
            piece += 1
        if pending is not None:
            count(*pending)
            pending = None
        for copy in copies:
            copy.wait()
        size = 2 * size
        if k <= nrow and size >= lanes:
            pending = (there, size // 2) if counted else (list(offset), size)
            counted = True
    count(*pending)

    per = frac.shape[0] // R
    sends = []
    for k, t in enumerate(row_peers):
        copy = pltpu.make_async_remote_copy(
            src_ref=frac.at[pl.ds(t * per, per)],
            dst_ref=fr_rows.at[R - 2 - k],
            send_sem=f_send.at[k], recv_sem=f_recv.at[R - 2 - k],
            device_id=(t, d), device_id_type=MESH,
        )
        copy.start()
        sends.append(copy)
    total = frac[pl.ds(r * per, per)]
    for k in range(R - 1):
        sends[k].wait_send()
        pltpu.make_async_remote_copy(
            src_ref=frac.at[pl.ds(r * per, per)],
            dst_ref=fr_rows.at[k], send_sem=f_send.at[k], recv_sem=f_recv.at[k],
            device_id=(row_peers[k], d), device_id_type=MESH,
        ).wait_recv()
        total = total + fr_rows[k]
    fr_sum[...] = total
    sends = []
    for k, t in enumerate(dim_peers):
        copy = pltpu.make_async_remote_copy(
            src_ref=fr_sum, dst_ref=fr_dim.at[k],
            send_sem=g_send.at[k], recv_sem=g_recv.at[k],
            device_id=(r, t), device_id_type=MESH,
        )
        copy.start()
        sends.append(copy)
    for k in range(N - 1):
        sends[k].wait_send()
        pltpu.make_async_remote_copy(
            src_ref=fr_sum, dst_ref=fr_dim.at[k],
            send_sem=g_send.at[k], recv_sem=g_recv.at[k],
            device_id=(r, dim_peers[k]), device_id_type=MESH,
        ).wait_recv()
        total = total + fr_dim[k]
    frac_out[...] = total
    own.wait()
    for copy in a2a:
        copy.wait()


def shards(entity_table, relations, thresholds, head_ids, rel_ids, thr_idx):
    R = lax.axis_size("rows")
    N = lax.axis_size("dim")
    n, width = entity_table.shape
    Q = head_ids.shape[0]
    blocks = Q // lanes
    per = blocks // R
    steps = bits_of(R) + bits_of(N)
    pieces = len(plan_for(N))
    f32 = jnp.float32
    DMA = pltpu.SemaphoreType.DMA
    smem = pl.BlockSpec(memory_space=pltpu.SMEM)
    vmem = pl.BlockSpec(memory_space=pltpu.VMEM)
    hbm = pl.BlockSpec(memory_space=pl.ANY)
    operands = [head_ids, rel_ids, thresholds, thr_idx.reshape(blocks, 1, lanes), relations, entity_table]
    if (width // N) % lanes:
        operands.append(entity_table.reshape(n, N, width // N).transpose(1, 0, 2))
    serving, share = pl.pallas_call(
        functools.partial(kernel, R, N, n * R * N),
        out_shape=(
            jax.ShapeDtypeStruct((n * N, width // N), f32),
            jax.ShapeDtypeStruct((per, 1, lanes), f32),
        ),
        in_specs=[smem, smem, smem, vmem, vmem] + [hbm] * (len(operands) - 5),
        out_specs=(hbm, vmem),
        scratch_shapes=[
            pltpu.VMEM((n, width), f32),
            pltpu.VMEM((n, width), jnp.bfloat16),
            pltpu.VMEM((Q, width), f32),
            pltpu.VMEM((Q, width), f32),
            pltpu.VMEM((Q, width), f32),
            pltpu.VMEM((2 * lanes, width), jnp.bfloat16),
            pltpu.VMEM((blocks, 1, lanes), f32),
            pltpu.VMEM((blocks, 1, lanes), f32),
            pltpu.VMEM((R - 1, per, 1, lanes), f32),
            pltpu.VMEM((N - 1, per, 1, lanes), f32),
            pltpu.VMEM((per, 1, lanes), f32),
            DMA, DMA,
            DMA((pieces, N - 1)), DMA((pieces, N - 1)),
            DMA((2, 2 * steps)), DMA((2, 2 * steps)),
            DMA((R - 1,)), DMA((R - 1,)),
            DMA((N - 1,)), DMA((N - 1,)),
        ],
        compiler_params=pltpu.CompilerParams(
            collective_id=0, has_side_effects=True, vmem_limit_bytes=60 * 2**20
        ),
    )(*operands)
    mine = Q // (R * N)
    fraction = lax.dynamic_slice(share.reshape(Q // R), (lax.axis_index("dim") * mine,), (mine,))
    return serving, fraction


def solution(mesh):
    placed = (P(("rows", "dim"), None), P(), P(), P(), P(), P())
    return jax.shard_map(
        shards,
        mesh=mesh,
        in_specs=placed,
        out_specs=(P("rows", "dim"), P(("rows", "dim"))),
        check_vma=False,
    )
```
